32 devices in a mesh: dp: 16 (over z, y, core), mp: 2 (over x).
Axes of the slice: x: 2, y: 2, z: 4, core: 2. Of those that a mesh axis runs over, the one named last changes fastest.
Arguments:
- inputs: bfloat16 [65536, 1024], P(('dp', 'mp')), may hold values from -6 to 6
- rand_blocks: int32 [16, 16, 62, 3], P('dp', 'mp'), may hold values from 1 to 62
- ln1_gain: float32 [1024], replicated, may hold values from 0.1 to 1.9
- ln1_bias: float32 [1024], replicated, may hold values from -4 to 4
- w_qkv: bfloat16 [3, 1024, 1024], P(None, None, 'mp'), may hold values from -0.1875 to 0.1875
- w_out: bfloat16 [1024, 1024], P('mp'), may hold values from -1.5 to 1.5
- ln2_gain: float32 [1024], replicated, may hold values from 0.1 to 1.9
- ln2_bias: float32 [1024], replicated, may hold values from -4 to 4
- w_up: bfloat16 [1024, 4096], P(None, 'mp'), may hold values from -0.1875 to 0.1875
- b_up: float32 [4096], P('mp'), may hold values from -6 to 6
- w_down: bfloat16 [4096, 1024], P('mp'), may hold values from -0.09375 to 0.09375
- b_down: float32 [1024], replicated, may hold values from -6 to 6
- cotangent: bfloat16 [65536, 1024], P(('dp', 'mp')), may hold values from -6 to 6
Outputs:
- output: float32 [65536, 1024], P(('dp', 'mp'))
- input_grad: float32 [65536, 1024], P(('dp', 'mp'))
- d_ln1_gain: float32 [1024], replicated
- d_ln1_bias: float32 [1024], replicated
- d_w_qkv: float32 [3, 1024, 1024], P(None, None, 'mp')
- d_w_out: float32 [1024, 1024], P('mp')
- d_ln2_gain: float32 [1024], replicated
- d_ln2_bias: float32 [1024], replicated
- d_w_up: float32 [1024, 4096], P(None, 'mp')
- d_b_up: float32 [4096], P('mp')
- d_w_down: float32 [4096, 1024], P('mp')
- d_b_down: float32 [1024], replicated
The draws below stay inside these ranges and needn't reach their ends.
Inputs may be any that keep to these rules, and one draw needn't show every extreme that they name: `rand_blocks`: a block may appear more than once in a list and may equal a window or global block.
All inputs are finite; a program needn't handle non-finite values.
Results may differ from the reference program's by a relative error of at most 0.02.
Values may be sent and summed in bfloat16 or wider, within the bound.
A program may use at most 320 MiB of HBM per device.

```python
from functools import partial
import jax
import jax.numpy as jnp
from jax import lax

D = 1024
HEADS = 16
HEAD_DIM = 64
FF = 4096
BLOCK = 64
RAND = 3
LEN = 4096
NB = 64
NSEQ = 16
TOKENS = 65536


def plant(drawn, key, low, top_value):
    spot = [jax.random.randint(jax.random.fold_in(key, axis), (), 0, length) for axis, length in enumerate(drawn.shape)]
    widest = drawn.shape.index(max(drawn.shape))
    next_to = spot[:widest] + [(spot[widest] + 1) % drawn.shape[widest]] + spot[widest + 1:]
    return drawn.at[tuple(spot)].set(low).at[tuple(next_to)].set(top_value)


def block_levels(key, shape, split, smallest, largest):
    def one(position, blocks):
        heights = jax.random.uniform(jax.random.fold_in(jax.random.fold_in(key, 6), position), (blocks,), jnp.float32, smallest / len(split), largest / len(split))
        return jnp.repeat(jnp.exp(heights), shape[position] // blocks).reshape((-1,) + (1,) * (len(shape) - position - 1))

    level = one(*split[0])
    for cut in split[1:]:
        level = level * one(*cut)
    return level


def normal_values(stream_key, dims, width, bound, shards=(), kind=jnp.bfloat16):
    gain = block_levels(stream_key, dims, shards, -0.22, 0.18) if shards else 1.0
    drawn = jax.random.normal(stream_key, dims, jnp.float32) * width * gain
    return jnp.minimum(jnp.maximum(drawn, -bound), bound).astype(kind)


def setup_inputs(seed: int = 0) -> dict:
    seeds = jax.random.split(jax.random.key(seed), 14)
    return {
        "inputs": normal_values(seeds[0], (TOKENS, D), 1.0, 6.0, ((0, 32),)),
        "rand_blocks": plant(jax.random.randint(seeds[1], (NSEQ, HEADS, NB - 2, RAND), 1, NB - 1), jax.random.fold_in(seeds[1], 1), 1, (NB - 1) - 1).astype(jnp.int32),
        "ln1_gain": jnp.clip(1.0 + 0.18 * jax.random.normal(seeds[2], (D,), jnp.float32), 0.1, 1.9),
        "ln1_bias": normal_values(seeds[3], (D,), 0.3, 4.0, (), jnp.float32),
        "w_qkv": normal_values(seeds[4], (3, D, D), D ** -0.5, 0.1875, ((2, 2),)),
        "w_out": normal_values(seeds[5], (D, D), (D // 64) ** -0.5, 1.5, ((0, 2),)),
        "ln2_gain": jnp.clip(1.0 + 0.18 * jax.random.normal(seeds[6], (D,), jnp.float32), 0.1, 1.9),
        "ln2_bias": normal_values(seeds[7], (D,), 0.3, 4.0, (), jnp.float32),
        "w_up": normal_values(seeds[8], (D, FF), D ** -0.5, 0.1875, ((1, 2),)),
        "b_up": normal_values(seeds[9], (FF,), 0.5, 6.0, ((0, 2),), jnp.float32),
        "w_down": normal_values(seeds[10], (FF, D), FF ** -0.5, 0.09375, ((0, 2),)),
        "b_down": normal_values(seeds[11], (D,), 0.5, 6.0, (), jnp.float32),
        "cotangent": normal_values(seeds[12], (TOKENS, D), 1.0, 6.0, ((0, 32),)),
    }


@jax.custom_vjp
def low(v):
    return lax.optimization_barrier(v.astype(jnp.bfloat16)).astype(jnp.float32)

@jax.custom_vjp
def low_back(v):
    return v

def low_keep(v):
    return (low(v), None)

def low_pass(kept, grad):
    return (grad,)

def back_keep(v):
    return (v, None)

def back_low(kept, grad):
    return (low(grad),)
low.defvjp(low_keep, low_pass)
low_back.defvjp(back_keep, back_low)
HIGH = lax.Precision.HIGHEST
EPSILON = 1e-05

def norm_rows(values, scale_vec, offset):
    centered = values - lax.optimization_barrier(jnp.mean(values, axis=-1, keepdims=True))
    inv_std = lax.rsqrt(lax.optimization_barrier(jnp.mean(centered * centered, axis=-1, keepdims=True)) + EPSILON)
    return centered * inv_std * scale_vec + offset

def block_table(random_rows, num_blocks):
    rows_idx = jnp.arange(num_blocks, dtype=jnp.int32)[:, None]
    steps_off = jnp.arange(-1, 2, dtype=jnp.int32)[None, :]
    window = jnp.clip(rows_idx + steps_off, 0, num_blocks - 1)
    filler = jnp.zeros((1, random_rows.shape[1]), jnp.int32)
    chosen = jnp.concatenate([filler, random_rows.astype(jnp.int32), filler], 0)
    first_cols = jnp.zeros((num_blocks, 1), jnp.int32)
    last_cols = first_cols + (num_blocks - 1)
    return jnp.concatenate([first_cols, last_cols, window, chosen], 1)

def head_attend(query, keys, values, table):
    num_blocks, per_query = table.shape
    seq_len, head_width = query.shape
    block_rows = seq_len // num_blocks
    scaling = head_width ** (-0.5)
    key_sets = keys.reshape(num_blocks, block_rows, head_width)[table].reshape(num_blocks, per_query * block_rows, head_width)
    value_sets = values.reshape(num_blocks, block_rows, head_width)[table].reshape(num_blocks, per_query * block_rows, head_width)
    query_sets = query.reshape(num_blocks, block_rows, head_width)
    scores = low_back(jnp.einsum('nqd,nkd->nqk', query_sets, key_sets, precision=HIGH) * scaling)
    mixed = jnp.einsum('nqk,nkd->nqd', low(jax.nn.softmax(scores, axis=-1)), value_sets, precision=HIGH)
    mixed = mixed.reshape(seq_len, head_width)
    end_rows = jnp.concatenate([query[:block_rows], query[seq_len - block_rows:]], 0)
    glob_scores = low_back(jnp.dot(end_rows, keys.T, precision=HIGH) * scaling)
    glob_mixed = jnp.dot(low(jax.nn.softmax(glob_scores, axis=-1)), values, precision=HIGH)
    mixed = mixed.at[:block_rows].set(glob_mixed[:block_rows])
    return mixed.at[seq_len - block_rows:].set(glob_mixed[block_rows:])

def attend_operands(operands):
    return head_attend(operands[0], operands[1], operands[2], operands[3])

def to_heads(matrix):
    return matrix.reshape(LEN, HEADS, HEAD_DIM).transpose(1, 0, 2)

def sequence_forward(params, operands):
    seq_in, rand_seq = operands
    ln1_gain, ln1_bias, w_qkv, w_out, ln2_gain, ln2_bias, w_up, b_up, w_down, b_down = params
    num_blocks = LEN // BLOCK
    first_rows = low(norm_rows(seq_in, ln1_gain, ln1_bias))
    projected = [low(low_back(jnp.dot(first_rows, w_qkv[index], precision=HIGH))) for index in range(3)]
    tables = jax.vmap(partial(block_table, num_blocks=num_blocks))(rand_seq)
    mixed = lax.map(jax.checkpoint(attend_operands), (to_heads(projected[0]), to_heads(projected[1]), to_heads(projected[2]), tables))
    attn_mix = low(low_back(mixed.transpose(1, 0, 2).reshape(LEN, D)))
    middle = seq_in + low_back(jnp.dot(attn_mix, w_out, precision=HIGH))
    second_rows = low(norm_rows(middle, ln2_gain, ln2_bias))
    hidden = low_back(jnp.dot(second_rows, w_up, precision=HIGH) + b_up)
    active = low(jax.nn.gelu(hidden, approximate=True))
    return middle + low_back(jnp.dot(active, w_down, precision=HIGH) + b_down)

def reference(inputs, rand_blocks, ln1_gain, ln1_bias, w_qkv, w_out, ln2_gain, ln2_bias, w_up, b_up, w_down, b_down, cotangent):
    num_seqs = rand_blocks.shape[0]
    params = tuple((param.astype(jnp.float32) for param in (ln1_gain, ln1_bias, w_qkv, w_out, ln2_gain, ln2_bias, w_up, b_up, w_down, b_down)))
    seqs_in = inputs.astype(jnp.float32).reshape(num_seqs, LEN, D)

    def whole(seqs_arg, params_arg):
        return lax.map(jax.checkpoint(partial(sequence_forward, params_arg)), (seqs_arg, rand_blocks))
    result, pullback = jax.vjp(whole, seqs_in, params)
    input_grad, grads = pullback(cotangent.astype(jnp.float32).reshape(num_seqs, LEN, D))
    return (result.reshape(num_seqs * LEN, D), input_grad.reshape(num_seqs * LEN, D), grads[0], grads[1], grads[2], grads[3], grads[4], grads[5], grads[6], grads[7], grads[8], grads[9])
```

```python
from functools import partial

import jax
import jax.numpy as jnp
from jax import lax
from jax.experimental import pallas as pl
from jax.experimental.pallas import tpu as pltpu
from jax.sharding import PartitionSpec as P

BLOCK = 64


EPSILON = 1e-05
PLAIN = (((1,), (1,)), ((), ()))
ROWWISE = (((0,), (0,)), ((), ()))
HIGH = lax.Precision.HIGHEST


def norm_rows(values, scale_vec, offset):
    centered = values - jnp.mean(values, axis=-1, keepdims=True)
    inv_std = lax.rsqrt(jnp.mean(centered * centered, axis=-1, keepdims=True) + EPSILON)
    normed = centered * inv_std
    return (normed * scale_vec + offset, normed, inv_std)


def norm_back(normed, inv_std, scale_vec, gradient):
    scaled = gradient * scale_vec
    inner_term = (
        scaled
        - jnp.mean(scaled, axis=-1, keepdims=True)
        - normed * jnp.mean(scaled * normed, axis=-1, keepdims=True)
    )
    return (inv_std * inner_term, jnp.sum(gradient * normed, 0), jnp.sum(gradient, 0))


def gelu_tanh(values):
    return jax.nn.gelu(values, approximate=True)


NT = (((1,), (1,)), ((), ()))
F32 = jnp.float32
BF16 = jnp.bfloat16
UNROLL_F = 2
UNROLL_B = 2


def mm(a, b):
    return jnp.dot(a, b, preferred_element_type=F32)


def mm_nt(a, b):
    return lax.dot_general(a, b, NT, preferred_element_type=F32)


def lane_left(rows, lanes=128):
    return lax.broadcasted_iota(jnp.int32, (rows, lanes), 1) % 128 < BLOCK


def fill_transposed(src_ref, out_ref, num_blocks):
    def one(j, c):
        t = src_ref[pl.ds(j * 128, 128), :].astype(F32).T
        out_ref[2 * j] = t.astype(BF16)
        out_ref[2 * j + 1] = pltpu.roll(t, BLOCK, 1).astype(BF16)
        return c
    lax.fori_loop(0, num_blocks // 2, one, 0, unroll=2)


def block_diag(x):
    left = lane_left(BLOCK)
    zero = jnp.zeros_like(x)
    return jnp.concatenate([jnp.where(left, x, zero), jnp.where(left, zero, x)], 0)


def rows_of(ref, b):
    return ref[pl.ds(pl.multiple_of(b * BLOCK, BLOCK), BLOCK), :]


def gather_rows(ref, i, pairs, num_blocks):
    left = lane_left(BLOCK)
    parts = [
        ref[0:BLOCK, :],
        ref[(num_blocks - 1) * BLOCK:, :],
        ref[pl.ds(pl.multiple_of((i - 1) * BLOCK, BLOCK), 3 * BLOCK), :],
    ]
    for a, b in pairs:
        parts.append(jnp.where(left, rows_of(ref, a), rows_of(ref, b)))
    return jnp.concatenate(parts, 0)


def gather_cols(tr, i, pairs, num_blocks):
    left = lane_left(128)

    def side(a, b):
        if a is b:
            return tr[a]
        return jnp.concatenate([tr[a, 0:BLOCK, :], tr[b, BLOCK:, :]], 0)

    def tile(first, second):
        return jnp.where(left, side(*first), side(second[0] ^ 1, second[1] ^ 1) if second[0] is not second[1] else tr[second[0] ^ 1])

    end = num_blocks - 1
    lo, hi = i - 1, i + 1
    r = pairs
    return jnp.concatenate([
        tile((0, 0), (end, end)),
        tile((lo, lo), (i, i)),
        tile((hi, hi), r[0]),
        tile(r[1], r[2]),
    ], 1)


def fwd_kernel(rand_ref, q_ref, k_ref, v_ref, o_ref, lse_ref, vt, *, scale):
    p = pl.program_id(0)
    num_blocks = q_ref.shape[0] // BLOCK
    fill_transposed(v_ref, vt, num_blocks)
    left = lane_left(BLOCK)
    inner = num_blocks - 2

    def qd(i):
        return block_diag(rows_of(q_ref, i) * jnp.asarray(scale, BF16))

    def finish(i, ot, m, l):
        o = (ot * (1.0 / l)).T
        o_ref[pl.ds(pl.multiple_of(i * BLOCK, BLOCK), BLOCK), :] = jnp.where(
            left, o[:BLOCK], o[BLOCK:]).astype(BF16)
        lse_ref[0, pl.ds(i, 1), :] = m + jnp.log(l)

    def regular(i):
        pairs = [(rand_ref[2 * p, (i - 1) * 3 + t], rand_ref[2 * p + 1, (i - 1) * 3 + t]) for t in range(3)]
        s = mm_nt(gather_rows(k_ref, i, pairs, num_blocks), qd(i))
        m = jnp.max(s, 0, keepdims=True)
        e = jnp.exp(s - m)
        l = jnp.sum(e, 0, keepdims=True)
        ot = mm(gather_cols(vt, i, pairs, num_blocks), e.astype(BF16))
        finish(i, ot, m, l)

    def step(n, c):
        for u in range(UNROLL_F):
            regular(1 + n * UNROLL_F + u)
        return c

    lax.fori_loop(0, inner // UNROLL_F, step, 0)
    for i in range(1 + inner // UNROLL_F * UNROLL_F, num_blocks - 1):
        regular(i)

    ends = (0, num_blocks - 1)
    qs = [qd(i) for i in ends]

    def chunk(c, carry):
        kc = k_ref[pl.ds(pl.multiple_of(c * 512, 512), 512), :]
        vc = jnp.concatenate([vt[c * 8 + 2 * t] for t in range(4)], 1)
        out = []
        for (m, l, acc), qb in zip(carry, qs):
            s = mm_nt(kc, qb)
            m2 = jnp.maximum(m, jnp.max(s, 0, keepdims=True))
            a = jnp.exp(m - m2)
            e = jnp.exp(s - m2)
            out.append((m2, l * a + jnp.sum(e, 0, keepdims=True), acc * a + mm(vc, e.astype(BF16))))
        return tuple(out)

    init = (jnp.full((1, 128), -jnp.inf, F32), jnp.zeros((1, 128), F32), jnp.zeros((128, 128), F32))
    res = lax.fori_loop(0, num_blocks * BLOCK // 512, chunk, (init, init))
    for i, (m, l, acc) in zip(ends, res):
        finish(i, acc, m, l)


def attend_fwd(rand2, qkv):
    rows, pairs = qkv.shape[1], qkv.shape[2] // 128
    num_blocks = rows // BLOCK

    def spec(which):
        return pl.BlockSpec((None, rows, 128), lambda p, r: (which, 0, p))

    return pl.pallas_call(
        partial(fwd_kernel, scale=BLOCK**-0.5),
        out_shape=(
            jax.ShapeDtypeStruct((rows, pairs * 128), BF16),
            jax.ShapeDtypeStruct((pairs, num_blocks, 128), F32),
        ),
        grid_spec=pltpu.PrefetchScalarGridSpec(
            num_scalar_prefetch=1,
            grid=(pairs,),
            in_specs=[spec(0), spec(1), spec(2)],
            out_specs=(
                pl.BlockSpec((rows, 128), lambda p, r: (0, p)),
                pl.BlockSpec((1, num_blocks, 128), lambda p, r: (p, 0, 0)),
            ),
            scratch_shapes=[pltpu.VMEM((num_blocks, 128, 128), BF16)],
        ),
        compiler_params=pltpu.CompilerParams(vmem_limit_bytes=60 << 20),
        cost_estimate=pl.CostEstimate(
            flops=pairs * num_blocks * 2 * 2 * 512 * 128 * 128,
            bytes_accessed=pairs * rows * 128 * 2 * 4,
            transcendentals=pairs * num_blocks * 512 * 128,
        ),
        name="attend_fwd",
    )(rand2, qkv, qkv, qkv)


def bwd_kernel(rand_ref, q_ref, k_ref, v_ref, do_ref, o_ref, lse_ref, out_ref, kt, acc, *, scale):
    p = pl.program_id(0)
    num_blocks = q_ref.shape[0] // BLOCK
    fill_transposed(k_ref, kt, num_blocks)
    left = lane_left(BLOCK)
    inner = num_blocks - 2
    sc = jnp.asarray(scale, BF16)
    acc[...] = jnp.zeros_like(acc)
    zero = jnp.zeros((BLOCK, 128), BF16)

    def operands(i):
        qi = rows_of(q_ref, i) * sc
        gi = rows_of(do_ref, i)
        ql, qr = jnp.where(left, qi, zero), jnp.where(left, zero, qi)
        gl, gr = jnp.where(left, gi, zero), jnp.where(left, zero, gi)
        qx = jnp.concatenate([qi[:, BLOCK:], qi[:, :BLOCK]], 1)
        gx = jnp.concatenate([gi[:, BLOCK:], gi[:, :BLOCK]], 1)
        score_rhs = jnp.concatenate([
            jnp.concatenate([ql, zero], 1), jnp.concatenate([qr, zero], 1),
            jnp.concatenate([zero, gl], 1), jnp.concatenate([zero, gr], 1)], 0)
        grad_rhs = jnp.concatenate([
            jnp.concatenate([gl, zero], 1), jnp.concatenate([zero, jnp.where(left, gx, zero)], 1),
            jnp.concatenate([jnp.where(left, zero, qx), zero], 1), jnp.concatenate([zero, qr], 1)], 0)
        return score_rhs, grad_rhs

    def grads(kv, score_rhs, grad_rhs, lse, delta):
        sd = mm_nt(kv, score_rhs)
        pr = jnp.exp(sd[:, :128] - lse)
        dp = sd[:, 128:]
        if delta is None:
            delta = jnp.sum(pr * dp, 0, keepdims=True)
        ds = (pr * (dp - delta)).astype(BF16)
        c = mm(jnp.concatenate([pr.astype(BF16), ds], 1), grad_rhs)
        return ds, c

    def put_dq(i, dqt):
        dq = dqt.T
        out_ref[0, pl.ds(pl.multiple_of(i * BLOCK, BLOCK), BLOCK), :] = (jnp.where(
            left, dq[:BLOCK], dq[BLOCK:]) * scale).astype(BF16)

    def regular(i):
        pairs = [(rand_ref[2 * p, (i - 1) * 3 + t], rand_ref[2 * p + 1, (i - 1) * 3 + t]) for t in range(3)]
        kv = jnp.concatenate([gather_rows(k_ref, i, pairs, num_blocks), gather_rows(v_ref, i, pairs, num_blocks)], 1)
        ds, c = grads(kv, *operands(i), lse_ref[0, pl.ds(i, 1), :], None)
        put_dq(i, mm(gather_cols(kt, i, pairs, num_blocks), ds))
        acc[0:BLOCK, :] += c[0:BLOCK]
        acc[(num_blocks - 1) * BLOCK:, :] += c[BLOCK:2 * BLOCK]
        acc[pl.ds(pl.multiple_of((i - 1) * BLOCK, BLOCK), 3 * BLOCK), :] += c[2 * BLOCK:5 * BLOCK]
        for t, (a, b) in enumerate(pairs):
            acc[pl.ds(pl.multiple_of(a * BLOCK, BLOCK), BLOCK), 0:128] += c[(5 + t) * BLOCK:(6 + t) * BLOCK, :128]
            acc[pl.ds(pl.multiple_of(b * BLOCK, BLOCK), BLOCK), 128:256] += c[(5 + t) * BLOCK:(6 + t) * BLOCK, 128:]

    def step(n, c):
        for u in range(UNROLL_B):
            regular(1 + n * UNROLL_B + u)
        return c

    lax.fori_loop(0, inner // UNROLL_B, step, 0)
    for i in range(1 + inner // UNROLL_B * UNROLL_B, num_blocks - 1):
        regular(i)

    for i in (0, num_blocks - 1):
        score_rhs, grad_rhs = operands(i)
        t = (rows_of(do_ref, i).astype(F32) * rows_of(o_ref, i).astype(F32)).T
        delta = jnp.concatenate([jnp.sum(t[:BLOCK], 0, keepdims=True), jnp.sum(t[BLOCK:], 0, keepdims=True)], 1)
        lse = lse_ref[0, i:i + 1, :]

        def chunk(c, dqt, score_rhs=score_rhs, grad_rhs=grad_rhs, lse=lse, delta=delta):
            at = pl.ds(pl.multiple_of(c * 512, 512), 512)
            kv = jnp.concatenate([k_ref[at, :], v_ref[at, :]], 1)
            ds, out = grads(kv, score_rhs, grad_rhs, lse, delta)
            acc[at, :] += out
            return dqt + mm(jnp.concatenate([kt[c * 8 + 2 * t] for t in range(4)], 1), ds)

        put_dq(i, lax.fori_loop(0, num_blocks * BLOCK // 512, chunk, jnp.zeros((128, 128), F32)))

    big = lane_left(512)

    def out(c, _):
        at = pl.ds(pl.multiple_of(c * 512, 512), 512)
        a0, a1 = acc[at, 0:128], acc[at, 128:256]
        out_ref[2, at, :] = jnp.where(big, a0, pltpu.roll(a1, BLOCK, 1)).astype(BF16)
        out_ref[1, at, :] = jnp.where(big, pltpu.roll(a0, BLOCK, 1), a1).astype(BF16)
        return _

    lax.fori_loop(0, num_blocks * BLOCK // 512, out, 0)


def attend_bwd(rand2, qkv, do, o, lse):
    rows, pairs = qkv.shape[1], qkv.shape[2] // 128
    num_blocks = rows // BLOCK

    def spec(which):
        return pl.BlockSpec((None, rows, 128), lambda p, r: (which, 0, p))

    flat = pl.BlockSpec((rows, 128), lambda p, r: (0, p))
    return pl.pallas_call(
        partial(bwd_kernel, scale=BLOCK**-0.5),
        out_shape=jax.ShapeDtypeStruct((3, rows, pairs * 128), BF16),
        grid_spec=pltpu.PrefetchScalarGridSpec(
            num_scalar_prefetch=1,
            grid=(pairs,),
            in_specs=[
                spec(0),
                spec(1),
                spec(2),
                flat,
                flat,
                pl.BlockSpec((1, num_blocks, 128), lambda p, r: (p, 0, 0)),
            ],
            out_specs=pl.BlockSpec((3, rows, 128), lambda p, r: (0, 0, p)),
            scratch_shapes=[
                pltpu.VMEM((num_blocks, 128, 128), BF16),
                pltpu.VMEM((rows, 256), F32),
            ],
        ),
        compiler_params=pltpu.CompilerParams(vmem_limit_bytes=60 << 20),
        cost_estimate=pl.CostEstimate(
            flops=pairs * num_blocks * 2 * 5 * 512 * 128 * 128,
            bytes_accessed=pairs * rows * 128 * 2 * 8,
            transcendentals=pairs * num_blocks * 512 * 128,
        ),
        name="attend_bwd",
    )(rand2, qkv, qkv, qkv, do, o, lse)


def per_device(
    inputs,
    rand_blocks,
    ln1_gain,
    ln1_bias,
    w_qkv,
    w_out,
    ln2_gain,
    ln2_bias,
    w_up,
    b_up,
    w_down,
    b_down,
    cotangent,
):
    seqs_here = rand_blocks.shape[0]
    heads_here = rand_blocks.shape[1]
    residual_in = inputs.astype(jnp.float32)
    normed_one, normed_a, inv_a = norm_rows(residual_in, ln1_gain, ln1_bias)
    first_rows = lax.all_gather(normed_one.astype(jnp.bfloat16), "mp", axis=0, tiled=True)
    group_rows = first_rows.shape[0]
    seq_len = group_rows // seqs_here
    projected = jnp.einsum(
        "td,cde->cte", first_rows, w_qkv, preferred_element_type=jnp.float32
    ).astype(jnp.bfloat16)
    tables = rand_blocks.reshape(seqs_here, heads_here, -1)
    qkv_seqs = [projected[:, n * seq_len : (n + 1) * seq_len] for n in range(seqs_here)]
    fwd_seqs = [attend_fwd(tables[n], qkv_seqs[n]) for n in range(seqs_here)]
    attn_mix = jnp.concatenate([o for o, _ in fwd_seqs], 0)
    attn_out = lax.psum_scatter(
        jnp.dot(attn_mix, w_out, preferred_element_type=jnp.float32).astype(jnp.bfloat16),
        "mp",
        scatter_dimension=0,
        tiled=True,
    ).astype(jnp.float32)
    mid_resid = residual_in + attn_out
    normed_two, normed_b, inv_b = norm_rows(mid_resid, ln2_gain, ln2_bias)
    second_rows, grad_rows = (
        lax.all_gather(normed_two.astype(jnp.bfloat16), "mp", axis=0, tiled=True),
        lax.all_gather(cotangent, "mp", axis=0, tiled=True),
    )
    hidden_pre = jnp.dot(second_rows, w_up, preferred_element_type=jnp.float32) + b_up
    hidden_act = gelu_tanh(hidden_pre).astype(jnp.bfloat16)
    branch_out = lax.psum_scatter(
        jnp.dot(hidden_act, w_down, preferred_element_type=jnp.float32).astype(jnp.bfloat16),
        "mp",
        scatter_dimension=0,
        tiled=True,
    ).astype(jnp.float32)
    result = mid_resid + (branch_out + b_down)
    grad_own = cotangent.astype(jnp.float32)
    bias_down_grad = jnp.sum(grad_own, 0)
    down_grad = lax.dot_general(hidden_act, grad_rows, ROWWISE, preferred_element_type=jnp.float32)
    act_grad = lax.dot_general(grad_rows, w_down, PLAIN, preferred_element_type=jnp.float32)
    gelu_pull = jax.vjp(gelu_tanh, hidden_pre)[1]
    pre_grad = gelu_pull(act_grad)[0].astype(jnp.bfloat16)
    bias_up_grad = jnp.sum(pre_grad.astype(jnp.float32), 0)
    up_grad = lax.dot_general(second_rows, pre_grad, ROWWISE, preferred_element_type=jnp.float32)
    second_grad = lax.psum_scatter(
        lax.dot_general(pre_grad, w_up, PLAIN, preferred_element_type=jnp.float32).astype(
            jnp.bfloat16
        ),
        "mp",
        scatter_dimension=0,
        tiled=True,
    ).astype(jnp.float32)
    mid_part, gain_two_grad, bias_two_grad = norm_back(normed_b, inv_b, ln2_gain, second_grad)
    mid_grad = grad_own + mid_part
    attn_grad_rows = lax.all_gather(mid_grad.astype(jnp.bfloat16), "mp", axis=0, tiled=True)
    out_grad = lax.dot_general(
        attn_mix, attn_grad_rows, ROWWISE, preferred_element_type=jnp.float32
    )
    mix_grad = lax.dot_general(
        attn_grad_rows, w_out, PLAIN, preferred_element_type=jnp.float32
    ).astype(jnp.bfloat16)
    stacked = jnp.concatenate(
        [
            attend_bwd(
                tables[n],
                qkv_seqs[n],
                mix_grad[n * seq_len : (n + 1) * seq_len],
                fwd_seqs[n][0],
                fwd_seqs[n][1],
            )
            for n in range(seqs_here)
        ],
        1,
    )
    qkv_grad = jnp.einsum("td,cte->cde", first_rows, stacked, preferred_element_type=jnp.float32)
    first_grad = lax.psum_scatter(
        jnp.einsum("cte,cde->td", stacked, w_qkv, preferred_element_type=jnp.float32).astype(
            jnp.bfloat16
        ),
        "mp",
        scatter_dimension=0,
        tiled=True,
    ).astype(jnp.float32)
    input_part, gain_one_grad, bias_one_grad = norm_back(normed_a, inv_a, ln1_gain, first_grad)
    input_grad = mid_grad + input_part
    small_sums = lax.psum(
        (gain_one_grad, bias_one_grad, gain_two_grad, bias_two_grad, bias_down_grad), ("dp", "mp")
    )
    qkv_grad, out_grad, up_grad, bias_up_grad, down_grad = (
        lax.psum(qkv_grad.astype(jnp.bfloat16), "dp").astype(jnp.float32),
        lax.psum(out_grad.astype(jnp.bfloat16), "dp").astype(jnp.float32),
        lax.psum(up_grad.astype(jnp.bfloat16), "dp").astype(jnp.float32),
        lax.psum(bias_up_grad.astype(jnp.bfloat16), "dp").astype(jnp.float32),
        lax.psum(down_grad.astype(jnp.bfloat16), "dp").astype(jnp.float32),
    )
    return (
        result,
        input_grad,
        small_sums[0],
        small_sums[1],
        qkv_grad,
        out_grad,
        small_sums[2],
        small_sums[3],
        up_grad,
        bias_up_grad,
        down_grad,
        small_sums[4],
    )


def solution(mesh):
    return jax.shard_map(
        per_device,
        mesh=mesh,
        in_specs=(
            P(("dp", "mp"), None),
            P("dp", "mp", None, None),
            P(),
            P(),
            P(None, None, "mp"),
            P("mp", None),
            P(),
            P(),
            P(None, "mp"),
            P("mp"),
            P("mp", None),
            P(),
            P(("dp", "mp"), None),
        ),
        out_specs=(
            P(("dp", "mp"), None),
            P(("dp", "mp"), None),
            P(),
            P(),
            P(None, None, "mp"),
            P("mp", None),
            P(),
            P(),
            P(None, "mp"),
            P("mp"),
            P("mp", None),
            P(),
        ),
        check_vma=False,
    )
```
